32 devices in a mesh: gx: 4 (over y, x), gy: 8 (over z, core).
Axes of the slice: x: 2, y: 2, z: 4, core: 2. Of those that a mesh axis runs over, the one named last changes fastest.
Arguments:
- tile_flux: bfloat16 [4, 12, 8, 131072], P(None, None, None, ('gx', 'gy')), may hold values from -6 to 6
- tile_frac: float32 [8, 131072], P(None, ('gx', 'gy')), may hold values from 0.02 to 1
- weights: bfloat16 [32, 7, 16, 256, 128], P(('gx', 'gy')), may hold values from -0.049804688 to 0.14941406
- block_row: int32 [32, 7, 16], P(('gx', 'gy')), may hold values from 0 to 47
- block_col: int32 [32, 7, 16], P(('gx', 'gy')), may hold values from 0 to 31
- send_counts: int32 [32, 7], P(('gx', 'gy')), may hold values from 1 to 16, as said below
Outputs:
- atm_flux: float32 [4, 12, 393216], P(None, None, ('gx', 'gy'))
The draws below stay inside these ranges and needn't reach their ends.
Inputs may be any that keep to these rules, and one draw needn't show every extreme that they name: `send_counts`: live slots of a device at an offset; some device has all 7 offsets at 16, and some device receives 16 live slots from every offset.
All inputs are finite; a program needn't handle non-finite values.
Results may differ from the reference program's by a relative error of at most 0.0029.
Values sent between devices are 32-bit elements; how exact they have to be, the bound alone decides.
A program may use at most 128 MiB of HBM per device.

```python
import math
import jax
import jax.numpy as jnp
from jax import lax

NFLUX = 12
TILES = 8
SUBSTEPS = 4
BROWS = 256
LCOLS = 128
REACH = 3
CAP = 16
LB_DEV = 32
AB_DEV = 48
NOFF = 7
LAND_CELLS = 131072
ATM_CELLS = 393216
DEVICES = 32


def draw_send_counts(key, part):
    key_base, key_full = jax.random.split(jax.random.fold_in(key, 17))
    base = jax.random.randint(key_base, (DEVICES, NOFF), 1, CAP // 2 + 1)
    full_dev = jax.random.randint(key_full, (), 0, DEVICES)
    row_ids = jnp.arange(DEVICES, dtype=jnp.int32)[:, None]
    col_ids = jnp.arange(NOFF, dtype=jnp.int32)[None, :]
    source = (full_dev - (col_ids - REACH)) % DEVICES
    filled = (row_ids == full_dev) | (row_ids == source)
    return jnp.where(filled, CAP, base).astype(jnp.int32)


def plant(values, key, least, top_value):
    spot = [jax.random.randint(jax.random.fold_in(key, axis), (), 0, length) for axis, length in enumerate(values.shape)]
    widest = values.shape.index(max(values.shape))
    next_to = spot[:widest] + [(spot[widest] + 1) % values.shape[widest]] + spot[widest + 1:]
    return values.at[tuple(spot)].set(least).at[tuple(next_to)].set(top_value)


def block_scale(own_key, extent, cuts, low, high):
    factor_of = 1.0
    for axis_at, shards_of in cuts:
        steps = jax.random.uniform(jax.random.fold_in(jax.random.fold_in(own_key, 6), axis_at), (shards_of,), jnp.float32, low / len(cuts), high / len(cuts))
        factor_of = factor_of * jnp.repeat(jnp.exp(steps), extent[axis_at] // shards_of).reshape((-1,) + (1,) * (len(extent) - 1 - axis_at))
    return factor_of


def bell_draw(stream_key, extent, spread, bound, cuts=(), held_as=jnp.bfloat16):
    result = spread * jax.random.normal(stream_key, extent, jnp.float32)
    if cuts:
        result = result * block_scale(stream_key, extent, cuts, -0.22, 0.18)
    return jnp.clip(result, -bound, bound).astype(held_as)


def setup_inputs(seed: int = 0) -> dict:
    streams_of = jax.random.split(jax.random.key(seed), 7)
    tile_flux = bell_draw(streams_of[0], (SUBSTEPS, NFLUX, TILES, LAND_CELLS), 1.0, 6.0, ((3, 32),))
    tile_frac = jnp.clip(jnp.exp(math.log(1.0) - 3.912023 * jax.random.uniform(streams_of[1], (TILES, LAND_CELLS), jnp.float32) ** block_scale(streams_of[1], (TILES, LAND_CELLS), ((1, 32),), -0.2, 0.2)), 0.02, 1.0)
    weights = jnp.clip(-0.049804688 + 0.19921875 * jax.random.uniform(streams_of[2], (DEVICES, NOFF, CAP, BROWS, LCOLS), jnp.float32) ** block_scale(streams_of[2], (DEVICES, NOFF, CAP, BROWS, LCOLS), ((0, 32),), -0.2, 0.2), -0.049804688, 0.14941406).astype(jnp.bfloat16)
    block_row = plant(jax.random.randint(streams_of[3], (DEVICES, NOFF, CAP), 0, AB_DEV), jax.random.fold_in(streams_of[3], 1), 0, AB_DEV - 1).astype(jnp.int32)
    block_col = plant(jax.random.randint(streams_of[4], (DEVICES, NOFF, CAP), 0, LB_DEV), jax.random.fold_in(streams_of[4], 1), 0, LB_DEV - 1).astype(jnp.int32)
    send_counts = draw_send_counts(jax.random.fold_in(streams_of[6], 71), 0)
    return {"tile_flux": tile_flux, "tile_frac": tile_frac, "weights": weights, "block_row": block_row, "block_col": block_col, "send_counts": send_counts}


def reference(tile_flux, tile_frac, weights, block_row, block_col, send_counts):
    frac_sum = jnp.sum(tile_frac, axis=0)
    merged = (jnp.sum(tile_flux.astype(jnp.float32) * tile_frac[None, None], axis=2) / frac_sum).astype(jnp.bfloat16)
    width = SUBSTEPS * NFLUX
    land_blocks = merged.reshape(width, DEVICES, LB_DEV, LCOLS).transpose(1, 2, 0, 3)

    def one_device(block_w, columns, counts, blocks):
        picked = blocks[columns]
        partial_value = jnp.einsum('okrc,okfc->okfr', block_w.astype(jnp.float32), picked.astype(jnp.float32))
        active = (jnp.arange(CAP, dtype=jnp.int32)[None, :] < counts[:, None]).astype(jnp.float32)
        return partial_value * active[:, :, None, None]

    def one_group(items):
        return jax.vmap(one_device)(*items)

    group = 8
    grouped = (weights.reshape((DEVICES // group, group) + weights.shape[1:]),
               block_col.reshape((DEVICES // group, group) + block_col.shape[1:]),
               send_counts.reshape((DEVICES // group, group) + send_counts.shape[1:]),
               land_blocks.reshape((DEVICES // group, group) + land_blocks.shape[1:]))
    partials = lax.map(one_group, grouped)
    dest_dev = (jnp.arange(DEVICES, dtype=jnp.int32)[:, None] + jnp.arange(NOFF, dtype=jnp.int32)[None, :] - REACH) % DEVICES
    target = (dest_dev[:, :, None] * AB_DEV + block_row).astype(jnp.int32)
    totals = jnp.zeros((DEVICES * AB_DEV, width, BROWS), jnp.float32)
    totals = totals.at[target.reshape(-1)].add(partials.reshape(-1, width, BROWS))
    return totals.transpose(1, 0, 2).reshape(SUBSTEPS, NFLUX, ATM_CELLS)
```

```python
import functools

import jax
import jax.numpy as jnp
from jax import lax
from jax.experimental import pallas as pl
from jax.experimental.pallas import tpu as pltpu
from jax.sharding import PartitionSpec as P

CHUNKS = 2


def send_order(num_off, reach):
    order = []
    for away in range(reach, 0, -1):
        order += [reach + away, reach - away]
    return order + [reach]


def exchange_kernel(axes, sizes, merged_ref, col_ref, count_ref, rows_ref, weights_ref,
                    arrived_ref, arrived_rows_ref,
                    weights_buf, part_buf, weight_sem, own_sem, send_sem, recv_sem,
                    row_send_sem, row_recv_sem):
    num_off, slots = weights_buf.shape[0], weights_buf.shape[1]
    reach = num_off // 2
    inner = sizes[1]
    count = sizes[0] * sizes[1]
    me = lax.axis_index(axes[0]) * inner + lax.axis_index(axes[1])
    order = send_order(num_off, reach)
    step = slots // CHUNKS

    def place(offset):
        there = lax.rem(me + offset - reach + count, count)
        return (there // inner, lax.rem(there, inner))

    loads = {}
    for offset in order:
        loads[offset] = pltpu.make_async_copy(
            weights_ref.at[offset], weights_buf.at[offset], weight_sem.at[offset])
        loads[offset].start()

    barrier = pltpu.get_barrier_semaphore()
    for offset in order[:-1]:
        pl.semaphore_signal(barrier, inc=1, device_id=place(offset),
                            device_id_type=pl.DeviceIdType.MESH)
    pl.semaphore_wait(barrier, num_off - 1)

    copies = []
    for offset in order:
        loads[offset].wait()
        if offset != reach:
            row_copy = pltpu.make_async_remote_copy(
                src_ref=rows_ref.at[offset], dst_ref=arrived_rows_ref.at[offset],
                send_sem=row_send_sem.at[offset], recv_sem=row_recv_sem.at[offset],
                device_id=place(offset), device_id_type=pl.DeviceIdType.MESH)
            row_copy.start()
            copies.append(row_copy)
        for chunk in range(CHUNKS):
            def one_slot(slot, carry, offset=offset):
                live = jnp.where(slot < count_ref[0, offset], 1.0, 0.0).astype(jnp.float32)
                picked = merged_ref[col_ref[0, offset, slot]]
                value = lax.dot_general(picked, weights_buf[offset, slot],
                                        (((1,), (1,)), ((), ())),
                                        preferred_element_type=jnp.float32)
                part_buf[offset, slot] = value * live
                return carry

            lax.fori_loop(chunk * step, (chunk + 1) * step, one_slot, 0)
            span = pl.ds(chunk * step, step)
            if offset != reach:
                copy = pltpu.make_async_remote_copy(
                    src_ref=part_buf.at[offset, span], dst_ref=arrived_ref.at[offset, span],
                    send_sem=send_sem.at[offset, chunk], recv_sem=recv_sem.at[offset, chunk],
                    device_id=place(offset), device_id_type=pl.DeviceIdType.MESH)
            else:
                copy = pltpu.make_async_copy(
                    part_buf.at[offset, span], arrived_ref.at[offset, span], own_sem.at[chunk])
            copy.start()
            copies.append(copy)
    own_rows = pltpu.make_async_copy(rows_ref.at[reach], arrived_rows_ref.at[reach],
                                     own_sem.at[CHUNKS])
    own_rows.start()
    copies.append(own_rows)
    for copy in copies:
        copy.wait()


def settle_kernel(rows_ref, arrived_ref, out_ref, arrived_buf, total, load_sem):
    num_off, slots = arrived_buf.shape[0], arrived_buf.shape[1]
    num_steps, num_kinds = out_ref.shape[0], out_ref.shape[1]
    blocks, block_rows = total.shape[0], total.shape[2]
    loads = []
    for offset in range(num_off):
        load = pltpu.make_async_copy(
            arrived_ref.at[offset], arrived_buf.at[offset], load_sem.at[offset])
        load.start()
        loads.append(load)
    total[...] = jnp.zeros_like(total)
    for offset in range(num_off):
        loads[offset].wait()

        def one_slot(slot, carry, offset=offset):
            row = rows_ref[offset, 0, slot]
            total[row] = total[row] + arrived_buf[offset, slot]
            return carry

        lax.fori_loop(0, slots, one_slot, 0)

    def one_block(block, carry):
        lanes = pl.ds(pl.multiple_of(block * block_rows, block_rows), block_rows)
        for step in range(num_steps):
            out_ref[step, :, lanes] = total[block, pl.ds(step * num_kinds, num_kinds), :]
        return carry

    lax.fori_loop(0, blocks, one_block, 0)


def on_device(axes, sizes, atm_blocks, tile_flux, tile_frac, weights, block_row, block_col,
              send_counts):
    num_steps, num_kinds = tile_flux.shape[0], tile_flux.shape[1]
    num_flux = num_steps * num_kinds
    num_off, slots, block_rows, block_cols = weights.shape[1:]
    frac_sum = jnp.sum(tile_frac, axis=0)
    merged = (
        jnp.sum(tile_flux.astype(jnp.float32) * tile_frac[None, None], axis=2) / frac_sum
    ).astype(jnp.bfloat16)
    land_blocks = merged.reshape(num_flux, -1, block_cols).transpose(1, 0, 2)
    rows = jnp.pad(block_row[0], ((0, 0), (0, 128 - slots))).reshape(num_off, 1, 128)

    smem = pl.BlockSpec(memory_space=pltpu.SMEM)
    vmem = pl.BlockSpec(memory_space=pltpu.VMEM)
    anywhere = pl.BlockSpec(memory_space=pl.ANY)
    arrived, arrived_rows = pl.pallas_call(
        functools.partial(exchange_kernel, axes, sizes),
        out_shape=(
            jax.ShapeDtypeStruct((num_off, slots, num_flux, block_rows), jnp.float32),
            jax.ShapeDtypeStruct((num_off, 1, 128), jnp.int32),
        ),
        in_specs=[vmem, smem, smem, anywhere, anywhere],
        out_specs=(anywhere, anywhere),
        scratch_shapes=[
            pltpu.VMEM(weights.shape[1:], weights.dtype),
            pltpu.VMEM((num_off, slots, num_flux, block_rows), jnp.float32),
            pltpu.SemaphoreType.DMA((num_off,)),
            pltpu.SemaphoreType.DMA((CHUNKS + 1,)),
            pltpu.SemaphoreType.DMA((num_off, CHUNKS)),
            pltpu.SemaphoreType.DMA((num_off, CHUNKS)),
            pltpu.SemaphoreType.DMA((num_off,)),
            pltpu.SemaphoreType.DMA((num_off,)),
        ],
        compiler_params=pltpu.CompilerParams(collective_id=0, has_side_effects=True),
        name="exchange",
    )(land_blocks, block_col, send_counts, rows, weights[0])

    return pl.pallas_call(
        settle_kernel,
        out_shape=jax.ShapeDtypeStruct((num_steps, num_kinds, atm_blocks * block_rows),
                                       jnp.float32),
        in_specs=[smem, anywhere],
        out_specs=vmem,
        scratch_shapes=[
            pltpu.VMEM((num_off, slots, num_flux, block_rows), jnp.float32),
            pltpu.VMEM((atm_blocks, num_flux, block_rows), jnp.float32),
            pltpu.SemaphoreType.DMA((num_off,)),
        ],
        name="settle",
    )(arrived_rows, arrived)


AB_DEV = 48


def solution(mesh):
    axes = ("gx", "gy")
    sizes = (mesh.shape["gx"], mesh.shape["gy"])
    return jax.shard_map(
        functools.partial(on_device, axes, sizes, AB_DEV),
        mesh=mesh,
        in_specs=(
            P(None, None, None, ("gx", "gy")),
            P(None, ("gx", "gy")),
            P(("gx", "gy"), None, None, None, None),
            P(("gx", "gy"), None, None),
            P(("gx", "gy"), None, None),
            P(("gx", "gy"), None),
        ),
        out_specs=P(None, None, ("gx", "gy")),
        check_vma=False,
    )
```

```python
import functools

import jax
import jax.numpy as jnp
from jax import lax
from jax.experimental import pallas as pl
from jax.experimental.pallas import tpu as pltpu
from jax.sharding import PartitionSpec as P

CUTS = 8
OUT_CUTS = 4


def chunk_spans(slots):
    spans, begin, size = [], 0, max(slots // CUTS, 1)
    while begin < slots:
        size = min(size if begin == 0 else begin, slots - begin)
        spans.append((begin, size))
        begin += size
    return spans


def send_order(reach, spans):
    order = []
    for away in range(reach, 0, -1):
        for chunk in range(len(spans)):
            order += [(reach + away, chunk), (reach - away, chunk)]
    return order + [(reach, chunk) for chunk in range(len(spans))]


def exchange_kernel(axes, sizes, spans, flux_ref, frac_ref, col_ref, count_ref, rows_ref,
                    weights_ref, arrived_ref, arrived_rows_ref,
                    flux_buf, frac_buf, weights_buf, part_buf, flux_sem, frac_sem, weight_sem,
                    own_sem, send_sem, recv_sem, row_send_sem, row_recv_sem):
    num_off, slots = weights_buf.shape[0], weights_buf.shape[1]
    num_steps, num_kinds, tiles, _ = flux_ref.shape
    cols = weights_buf.shape[3]
    reach = num_off // 2
    inner = sizes[1]
    count = sizes[0] * sizes[1]
    me = lax.axis_index(axes[0]) * inner + lax.axis_index(axes[1])
    order = send_order(reach, spans)

    def place(offset):
        there = lax.rem(me + offset - reach + count, count)
        return (there // inner, lax.rem(there, inner))

    land_loads = []
    for block in range(flux_buf.shape[0]):
        lanes = pl.ds(block * cols, cols)
        land_loads.append(pltpu.make_async_copy(
            flux_ref.at[:, :, :, lanes], flux_buf.at[block], flux_sem.at[block]))
        land_loads.append(pltpu.make_async_copy(
            frac_ref.at[:, lanes], frac_buf.at[block], frac_sem.at[block]))
    for load in land_loads:
        load.start()
    loads = {}
    for offset, chunk in order:
        if offset not in loads:
            loads[offset] = pltpu.make_async_copy(
                weights_ref.at[offset], weights_buf.at[offset], weight_sem.at[offset])
            loads[offset].start()

    barrier = pltpu.get_barrier_semaphore()
    for offset in range(num_off):
        if offset != reach:
            pl.semaphore_signal(barrier, inc=1, device_id=place(offset),
                                device_id_type=pl.DeviceIdType.MESH)
    pl.semaphore_wait(barrier, num_off - 1)

    for load in land_loads:
        load.wait()
    copies = []
    loaded = set()
    for offset, chunk in order:
        begin, size = spans[chunk]
        if offset not in loaded:
            loads[offset].wait()
            loaded.add(offset)

        def one_slot(slot, carry, offset=offset):
            live = jnp.where(slot < count_ref[0, offset], 1.0, 0.0).astype(jnp.float32)
            block = col_ref[offset, 0, slot]
            frac = frac_buf[block]
            flux = flux_buf[block].astype(jnp.float32)
            flux = jnp.stack([flux[step] for step in range(num_steps)], axis=1)
            flux = flux.reshape(num_steps * num_kinds, tiles, cols)
            merged = jnp.sum(flux * frac[None], axis=1) / jnp.sum(frac, axis=0, keepdims=True)
            value = lax.dot_general(merged.astype(jnp.bfloat16), weights_buf[offset, slot],
                                    (((1,), (1,)), ((), ())),
                                    preferred_element_type=jnp.float32)
            part_buf[offset, slot] = value * live
            return carry

        lax.fori_loop(begin, begin + size, one_slot, 0)
        span = pl.ds(begin, size)
        if offset != reach:
            copy = pltpu.make_async_remote_copy(
                src_ref=part_buf.at[offset, span], dst_ref=arrived_ref.at[offset, span],
                send_sem=send_sem.at[offset, chunk], recv_sem=recv_sem.at[offset, chunk],
                device_id=place(offset), device_id_type=pl.DeviceIdType.MESH)
        else:
            copy = pltpu.make_async_copy(
                part_buf.at[offset, span], arrived_ref.at[offset, span], own_sem.at[chunk])
        copy.start()
        copies.append(copy)
        if chunk == 0:
            if offset != reach:
                copy = pltpu.make_async_remote_copy(
                    src_ref=rows_ref.at[offset], dst_ref=arrived_rows_ref.at[offset],
                    send_sem=row_send_sem.at[offset], recv_sem=row_recv_sem.at[offset],
                    device_id=place(offset), device_id_type=pl.DeviceIdType.MESH)
            else:
                copy = pltpu.make_async_copy(
                    rows_ref.at[reach], arrived_rows_ref.at[reach], own_sem.at[len(spans)])
            copy.start()
            copies.append(copy)
    for copy in copies:
        copy.wait()


def settle_kernel(rows_ref, arrived_ref, out_ref, arrived_buf, total, out_buf, load_sem,
                  out_sem):
    num_off, slots = arrived_buf.shape[0], arrived_buf.shape[1]
    num_kinds, num_steps = out_ref.shape[0], out_ref.shape[1]
    blocks, _, block_rows = total.shape
    loads = []
    for offset in range(num_off):
        load = pltpu.make_async_copy(
            arrived_ref.at[offset], arrived_buf.at[offset], load_sem.at[offset])
        load.start()
        loads.append(load)
    total[...] = jnp.zeros_like(total)
    for offset in range(num_off):
        loads[offset].wait()

        def one_slot(slot, carry, offset=offset):
            row = rows_ref[offset, 0, slot]
            total[row] = total[row] + arrived_buf[offset, slot]
            return carry

        lax.fori_loop(0, slots, one_slot, 0, unroll=4)

    per_cut = blocks // OUT_CUTS
    stores = []
    for cut in range(OUT_CUTS):
        def one_block(block, carry):
            lanes = pl.ds(pl.multiple_of(block * block_rows, block_rows), block_rows)
            out_buf[:, :, lanes] = total[block].reshape(num_kinds, num_steps, block_rows)
            return carry

        lax.fori_loop(cut * per_cut, (cut + 1) * per_cut, one_block, 0, unroll=2)
        lanes = pl.ds(cut * per_cut * block_rows, per_cut * block_rows)
        store = pltpu.make_async_copy(
            out_buf.at[:, :, lanes], out_ref.at[:, :, lanes], out_sem.at[cut])
        store.start()
        stores.append(store)
    for store in stores:
        store.wait()


def on_device(axes, sizes, atm_blocks, tile_flux, tile_frac, weights, block_row, block_col,
              send_counts):
    num_steps, num_kinds = tile_flux.shape[0], tile_flux.shape[1]
    num_flux = num_steps * num_kinds
    num_off, slots, block_rows, block_cols = weights.shape[1:]
    tiles = tile_flux.shape[2]
    land_blocks = tile_flux.shape[3] // block_cols
    spans = chunk_spans(slots)
    rows = block_row.transpose(1, 0, 2)
    columns = block_col.transpose(1, 0, 2)

    smem = pl.BlockSpec(memory_space=pltpu.SMEM)
    anywhere = pl.BlockSpec(memory_space=pl.ANY)
    arrived, arrived_rows = pl.pallas_call(
        functools.partial(exchange_kernel, axes, sizes, spans),
        out_shape=(
            jax.ShapeDtypeStruct((num_off, slots, num_flux, block_rows), jnp.float32),
            jax.ShapeDtypeStruct(rows.shape, jnp.int32),
        ),
        in_specs=[anywhere, anywhere, smem, smem, anywhere, anywhere],
        out_specs=(anywhere, anywhere),
        scratch_shapes=[
            pltpu.VMEM((land_blocks, num_steps, num_kinds, tiles, block_cols), tile_flux.dtype),
            pltpu.VMEM((land_blocks, tiles, block_cols), tile_frac.dtype),
            pltpu.VMEM(weights.shape[1:], weights.dtype),
            pltpu.VMEM((num_off, slots, num_flux, block_rows), jnp.float32),
            pltpu.SemaphoreType.DMA((land_blocks,)),
            pltpu.SemaphoreType.DMA((land_blocks,)),
            pltpu.SemaphoreType.DMA((num_off,)),
            pltpu.SemaphoreType.DMA((len(spans) + 1,)),
            pltpu.SemaphoreType.DMA((num_off, len(spans))),
            pltpu.SemaphoreType.DMA((num_off, len(spans))),
            pltpu.SemaphoreType.DMA((num_off,)),
            pltpu.SemaphoreType.DMA((num_off,)),
        ],
        compiler_params=pltpu.CompilerParams(collective_id=0, has_side_effects=True),
        name="exchange",
    )(tile_flux, tile_frac, columns, send_counts, rows, weights[0])

    out = pl.pallas_call(
        settle_kernel,
        out_shape=jax.ShapeDtypeStruct((num_kinds, num_steps, atm_blocks * block_rows),
                                       jnp.float32),
        in_specs=[smem, anywhere],
        out_specs=anywhere,
        scratch_shapes=[
            pltpu.VMEM((num_off, slots, num_flux, block_rows), jnp.float32),
            pltpu.VMEM((atm_blocks, num_flux, block_rows), jnp.float32),
            pltpu.VMEM((num_kinds, num_steps, atm_blocks * block_rows), jnp.float32),
            pltpu.SemaphoreType.DMA((num_off,)),
            pltpu.SemaphoreType.DMA((OUT_CUTS,)),
        ],
        name="settle",
    )(arrived_rows, arrived)
    return out.transpose(1, 0, 2)


AB_DEV = 48


def solution(mesh):
    axes = ("gx", "gy")
    sizes = (mesh.shape["gx"], mesh.shape["gy"])
    return jax.shard_map(
        functools.partial(on_device, axes, sizes, AB_DEV),
        mesh=mesh,
        in_specs=(
            P(None, None, None, ("gx", "gy")),
            P(None, ("gx", "gy")),
            P(("gx", "gy"), None, None, None, None),
            P(("gx", "gy"), None, None),
            P(("gx", "gy"), None, None),
            P(("gx", "gy"), None),
        ),
        out_specs=P(None, None, ("gx", "gy")),
        check_vma=False,
    )
```

```python
import functools

import jax
import jax.numpy as jnp
from jax import lax
from jax.experimental import pallas as pl
from jax.experimental.pallas import tpu as pltpu
from jax.sharding import PartitionSpec as P

CUTS = 8
OUT_CUTS = 4


def chunk_spans(slots):
    spans, begin, size = [], 0, max(slots // CUTS, 1)
    while begin < slots:
        size = min(size if begin == 0 else begin, slots - begin)
        spans.append((begin, size))
        begin += size
    return spans


def send_order(reach, spans):
    order = []
    for away in range(reach, 0, -1):
        for chunk in range(len(spans)):
            order += [(reach + away, chunk), (reach - away, chunk)]
    return order + [(reach, chunk) for chunk in range(len(spans))]


def exchange_kernel(axes, sizes, spans, flux_ref, frac_ref, col_ref, count_ref, rows_ref,
                    weights_ref, arrived_ref, arrived_rows_ref,
                    flux_buf, frac_buf, weights_buf, part_buf, flux_sem, frac_sem, weight_sem,
                    own_sem, send_sem, recv_sem, row_send_sem, row_recv_sem):
    num_off, slots = weights_buf.shape[0], weights_buf.shape[1]
    num_steps, num_kinds, tiles, _ = flux_ref.shape
    cols = weights_buf.shape[3]
    reach = num_off // 2
    inner = sizes[1]
    count = sizes[0] * sizes[1]
    me = lax.axis_index(axes[0]) * inner + lax.axis_index(axes[1])
    order = send_order(reach, spans)

    def place(offset):
        there = lax.rem(me + offset - reach + count, count)
        return (there // inner, lax.rem(there, inner))

    barrier = pltpu.get_barrier_semaphore()
    for offset in range(num_off):
        if offset != reach:
            pl.semaphore_signal(barrier, inc=1, device_id=place(offset),
                                device_id_type=pl.DeviceIdType.MESH)

    land_loads = []
    for block in range(flux_buf.shape[0]):
        lanes = pl.ds(block * cols, cols)
        land_loads.append(pltpu.make_async_copy(
            flux_ref.at[:, :, :, lanes], flux_buf.at[block], flux_sem.at[block]))
        land_loads.append(pltpu.make_async_copy(
            frac_ref.at[:, lanes], frac_buf.at[block], frac_sem.at[block]))
    for load in land_loads:
        load.start()
    loads = {}
    for offset, chunk in order:
        if offset not in loads:
            loads[offset] = pltpu.make_async_copy(
                weights_ref.at[offset], weights_buf.at[offset], weight_sem.at[offset])
            loads[offset].start()

    for load in land_loads:
        load.wait()
    copies = []
    loaded = set()
    for offset, chunk in order:
        begin, size = spans[chunk]
        if offset not in loaded:
            loads[offset].wait()
            loaded.add(offset)

        def one_slot(slot, carry, offset=offset):
            live = jnp.where(slot < count_ref[0, offset], 1.0, 0.0).astype(jnp.float32)
            block = col_ref[offset, 0, slot]
            frac = frac_buf[block]
            flux = flux_buf[block].astype(jnp.float32)
            flux = jnp.stack([flux[step] for step in range(num_steps)], axis=1)
            flux = flux.reshape(num_steps * num_kinds, tiles, cols)
            merged = jnp.sum(flux * frac[None], axis=1) / jnp.sum(frac, axis=0, keepdims=True)
            value = lax.dot_general(merged.astype(jnp.bfloat16), weights_buf[offset, slot],
                                    (((1,), (1,)), ((), ())),
                                    preferred_element_type=jnp.float32)
            part_buf[offset, slot] = value * live
            return carry

        lax.fori_loop(begin, begin + size, one_slot, 0)
        if not copies:
            pl.semaphore_wait(barrier, num_off - 1)
        span = pl.ds(begin, size)
        if offset != reach:
            copy = pltpu.make_async_remote_copy(
                src_ref=part_buf.at[offset, span], dst_ref=arrived_ref.at[offset, span],
                send_sem=send_sem.at[offset, chunk], recv_sem=recv_sem.at[offset, chunk],
                device_id=place(offset), device_id_type=pl.DeviceIdType.MESH)
        else:
            copy = pltpu.make_async_copy(
                part_buf.at[offset, span], arrived_ref.at[offset, span], own_sem.at[chunk])
        copy.start()
        copies.append(copy)
        if chunk == 0:
            if offset != reach:
                copy = pltpu.make_async_remote_copy(
                    src_ref=rows_ref.at[offset], dst_ref=arrived_rows_ref.at[offset],
                    send_sem=row_send_sem.at[offset], recv_sem=row_recv_sem.at[offset],
                    device_id=place(offset), device_id_type=pl.DeviceIdType.MESH)
            else:
                copy = pltpu.make_async_copy(
                    rows_ref.at[reach], arrived_rows_ref.at[reach], own_sem.at[len(spans)])
            copy.start()
            copies.append(copy)
    for copy in copies:
        copy.wait()


def settle_kernel(rows_ref, arrived_ref, out_ref, rows, total, out_buf, load_sem, out_sem):
    num_off, slots = arrived_ref.shape[0], arrived_ref.shape[1]
    num_kinds, num_steps = out_ref.shape[0], out_ref.shape[1]
    blocks, _, block_rows = total.shape
    load = pltpu.make_async_copy(rows_ref, rows, load_sem)
    load.start()
    total[...] = jnp.zeros_like(total)
    load.wait()
    for offset in range(num_off):
        def one_slot(slot, carry, offset=offset):
            row = rows[offset, 0, slot]
            total[row] = total[row] + arrived_ref[offset, slot]
            return carry

        lax.fori_loop(0, slots, one_slot, 0, unroll=4)

    per_cut = blocks // OUT_CUTS
    stores = []
    for cut in range(OUT_CUTS):
        def one_block(block, carry):
            lanes = pl.ds(pl.multiple_of(block * block_rows, block_rows), block_rows)
            out_buf[:, :, lanes] = total[block].reshape(num_kinds, num_steps, block_rows)
            return carry

        lax.fori_loop(cut * per_cut, (cut + 1) * per_cut, one_block, 0, unroll=2)
        lanes = pl.ds(cut * per_cut * block_rows, per_cut * block_rows)
        store = pltpu.make_async_copy(
            out_buf.at[:, :, lanes], out_ref.at[:, :, lanes], out_sem.at[cut])
        store.start()
        stores.append(store)
    for store in stores:
        store.wait()


def on_device(axes, sizes, atm_blocks, tile_flux, tile_frac, weights, block_row, block_col,
              send_counts):
    num_steps, num_kinds = tile_flux.shape[0], tile_flux.shape[1]
    num_flux = num_steps * num_kinds
    num_off, slots, block_rows, block_cols = weights.shape[1:]
    tiles = tile_flux.shape[2]
    land_blocks = tile_flux.shape[3] // block_cols
    spans = chunk_spans(slots)
    rows = block_row.transpose(1, 0, 2)
    columns = block_col.transpose(1, 0, 2)

    vmem = pl.BlockSpec(memory_space=pltpu.VMEM)
    smem = pl.BlockSpec(memory_space=pltpu.SMEM)
    hbm = pl.BlockSpec(memory_space=pltpu.HBM)
    arrived, arrived_rows = pl.pallas_call(
        functools.partial(exchange_kernel, axes, sizes, spans),
        out_shape=(
            pltpu.VMEM((num_off, slots, num_flux, block_rows), jnp.float32),
            pltpu.VMEM(rows.shape, jnp.int32),
        ),
        in_specs=[hbm, hbm, smem, smem, hbm, hbm],
        out_specs=(vmem, vmem),
        scratch_shapes=[
            pltpu.VMEM((land_blocks, num_steps, num_kinds, tiles, block_cols), tile_flux.dtype),
            pltpu.VMEM((land_blocks, tiles, block_cols), tile_frac.dtype),
            pltpu.VMEM(weights.shape[1:], weights.dtype),
            pltpu.VMEM((num_off, slots, num_flux, block_rows), jnp.float32),
            pltpu.SemaphoreType.DMA((land_blocks,)),
            pltpu.SemaphoreType.DMA((land_blocks,)),
            pltpu.SemaphoreType.DMA((num_off,)),
            pltpu.SemaphoreType.DMA((len(spans) + 1,)),
            pltpu.SemaphoreType.DMA((num_off, len(spans))),
            pltpu.SemaphoreType.DMA((num_off, len(spans))),
            pltpu.SemaphoreType.DMA((num_off,)),
            pltpu.SemaphoreType.DMA((num_off,)),
        ],
        compiler_params=pltpu.CompilerParams(collective_id=0, has_side_effects=True,
                                             vmem_limit_bytes=57 * 2**20),
        name="exchange",
    )(tile_flux, tile_frac, columns, send_counts, rows, weights[0])

    out = pl.pallas_call(
        settle_kernel,
        out_shape=jax.ShapeDtypeStruct((num_kinds, num_steps, atm_blocks * block_rows),
                                       jnp.float32),
        in_specs=[vmem, vmem],
        out_specs=hbm,
        scratch_shapes=[
            pltpu.SMEM(rows.shape, jnp.int32),
            pltpu.VMEM((atm_blocks, num_flux, block_rows), jnp.float32),
            pltpu.VMEM((num_kinds, num_steps, atm_blocks * block_rows), jnp.float32),
            pltpu.SemaphoreType.DMA,
            pltpu.SemaphoreType.DMA((OUT_CUTS,)),
        ],
        compiler_params=pltpu.CompilerParams(vmem_limit_bytes=16 * 2**20),
        name="settle",
    )(arrived_rows, arrived)
    return out.transpose(1, 0, 2)


AB_DEV = 48


def solution(mesh):
    axes = ("gx", "gy")
    sizes = (mesh.shape["gx"], mesh.shape["gy"])
    return jax.shard_map(
        functools.partial(on_device, axes, sizes, AB_DEV),
        mesh=mesh,
        in_specs=(
            P(None, None, None, ("gx", "gy")),
            P(None, ("gx", "gy")),
            P(("gx", "gy"), None, None, None, None),
            P(("gx", "gy"), None, None),
            P(("gx", "gy"), None, None),
            P(("gx", "gy"), None),
        ),
        out_specs=P(None, None, ("gx", "gy")),
        check_vma=False,
    )
```

```python
import functools

import jax
import jax.numpy as jnp
from jax import lax
from jax.experimental import pallas as pl
from jax.experimental.pallas import tpu as pltpu
from jax.sharding import PartitionSpec as P

CUTS = 8
OUT_CUTS = 4
EARLY = 4


def chunk_spans(slots):
    spans, begin, size = [], 0, max(slots // CUTS, 1)
    while begin < slots:
        size = min(size if begin == 0 else begin, slots - begin)
        spans.append((begin, size))
        begin += size
    return spans


def send_order(reach, spans):
    order = []
    for away in range(reach, 0, -1):
        for chunk in range(len(spans)):
            order += [(reach + away, chunk), (reach - away, chunk)]
    return order + [(reach, chunk) for chunk in range(len(spans))]


def exchange_kernel(axes, sizes, spans, flux_ref, frac_ref, col_ref, count_ref, rows_ref,
                    weights_ref, arrived_ref, arrived_rows_ref,
                    flux_buf, frac_buf, weights_buf, part_buf, flux_sem, frac_sem, weight_sem,
                    own_sem, send_sem, recv_sem, row_send_sem, row_recv_sem):
    num_off, slots = weights_buf.shape[0], weights_buf.shape[1]
    num_steps, num_kinds, tiles, _ = flux_ref.shape
    cols = weights_buf.shape[3]
    reach = num_off // 2
    inner = sizes[1]
    count = sizes[0] * sizes[1]
    me = lax.axis_index(axes[0]) * inner + lax.axis_index(axes[1])
    order = send_order(reach, spans)

    def place(offset):
        there = lax.rem(me + offset - reach + count, count)
        return (there // inner, lax.rem(there, inner))

    barrier = pltpu.get_barrier_semaphore()
    for offset in range(num_off):
        if offset != reach:
            pl.semaphore_signal(barrier, inc=1, device_id=place(offset),
                                device_id_type=pl.DeviceIdType.MESH)

    land_loads = []
    for block in range(flux_buf.shape[0]):
        lanes = pl.ds(block * cols, cols)
        land_loads.append(pltpu.make_async_copy(
            flux_ref.at[:, :, :, lanes], flux_buf.at[block], flux_sem.at[block]))
        land_loads.append(pltpu.make_async_copy(
            frac_ref.at[:, lanes], frac_buf.at[block], frac_sem.at[block]))
    for load in land_loads:
        load.start()
    loads = {}
    for offset, chunk in order:
        span = pl.ds(*spans[chunk])
        loads[offset, chunk] = pltpu.make_async_copy(
            weights_ref.at[offset, span], weights_buf.at[offset, span],
            weight_sem.at[offset, chunk])
    for key in order[:EARLY]:
        loads[key].start()

    for load in land_loads:
        load.wait()
    for key in order[EARLY:]:
        loads[key].start()
    copies = []
    for offset, chunk in order:
        begin, size = spans[chunk]
        loads[offset, chunk].wait()
        part_ref = arrived_ref if offset == reach else part_buf

        def one_slot(slot, carry, offset=offset, part_ref=part_ref):
            live = jnp.where(slot < count_ref[0, offset], 1.0, 0.0).astype(jnp.float32)
            block = col_ref[offset, 0, slot]
            frac = frac_buf[block]
            flux = flux_buf[block].astype(jnp.float32)
            flux = jnp.stack([flux[step] for step in range(num_steps)], axis=1)
            flux = flux.reshape(num_steps * num_kinds, tiles, cols)
            merged = jnp.sum(flux * frac[None], axis=1) / jnp.sum(frac, axis=0, keepdims=True)
            value = lax.dot_general(merged.astype(jnp.bfloat16), weights_buf[offset, slot],
                                    (((1,), (1,)), ((), ())),
                                    preferred_element_type=jnp.float32)
            part_ref[offset, slot] = value * live
            return carry

        lax.fori_loop(begin, begin + size, one_slot, 0)
        if not copies:
            pl.semaphore_wait(barrier, num_off - 1)
        span = pl.ds(begin, size)
        if offset != reach:
            copy = pltpu.make_async_remote_copy(
                src_ref=part_buf.at[offset, span], dst_ref=arrived_ref.at[offset, span],
                send_sem=send_sem.at[offset, chunk], recv_sem=recv_sem.at[offset, chunk],
                device_id=place(offset), device_id_type=pl.DeviceIdType.MESH)
            copy.start()
            copies.append(copy)
        if chunk == 0:
            if offset != reach:
                copy = pltpu.make_async_remote_copy(
                    src_ref=rows_ref.at[offset], dst_ref=arrived_rows_ref.at[offset],
                    send_sem=row_send_sem.at[offset], recv_sem=row_recv_sem.at[offset],
                    device_id=place(offset), device_id_type=pl.DeviceIdType.MESH)
            else:
                copy = pltpu.make_async_copy(
                    rows_ref.at[reach], arrived_rows_ref.at[reach], own_sem)
            copy.start()
            copies.append(copy)
    for copy in copies:
        copy.wait()


def settle_kernel(rows_ref, arrived_ref, out_ref, rows, total, out_buf, load_sem, out_sem):
    num_off, slots = arrived_ref.shape[0], arrived_ref.shape[1]
    num_kinds, num_steps = out_ref.shape[0], out_ref.shape[1]
    blocks, _, block_rows = total.shape
    load = pltpu.make_async_copy(rows_ref, rows, load_sem)
    load.start()
    total[...] = jnp.zeros_like(total)
    load.wait()
    for offset in range(num_off):
        def one_slot(slot, carry, offset=offset):
            row = rows[offset, 0, slot]
            total[row] = total[row] + arrived_ref[offset, slot]
            return carry

        lax.fori_loop(0, slots, one_slot, 0, unroll=4)

    per_cut = blocks // OUT_CUTS
    stores = []
    for cut in range(OUT_CUTS):
        def one_block(block, carry):
            lanes = pl.ds(pl.multiple_of(block * block_rows, block_rows), block_rows)
            out_buf[:, :, lanes] = total[block].reshape(num_kinds, num_steps, block_rows)
            return carry

        lax.fori_loop(cut * per_cut, (cut + 1) * per_cut, one_block, 0, unroll=2)
        lanes = pl.ds(cut * per_cut * block_rows, per_cut * block_rows)
        store = pltpu.make_async_copy(
            out_buf.at[:, :, lanes], out_ref.at[:, :, lanes], out_sem.at[cut])
        store.start()
        stores.append(store)
    for store in stores:
        store.wait()


def on_device(axes, sizes, atm_blocks, tile_flux, tile_frac, weights, block_row, block_col,
              send_counts):
    num_steps, num_kinds = tile_flux.shape[0], tile_flux.shape[1]
    num_flux = num_steps * num_kinds
    num_off, slots, block_rows, block_cols = weights.shape[1:]
    tiles = tile_flux.shape[2]
    land_blocks = tile_flux.shape[3] // block_cols
    spans = chunk_spans(slots)
    rows = block_row.transpose(1, 0, 2)
    columns = block_col.transpose(1, 0, 2)

    vmem = pl.BlockSpec(memory_space=pltpu.VMEM)
    smem = pl.BlockSpec(memory_space=pltpu.SMEM)
    hbm = pl.BlockSpec(memory_space=pltpu.HBM)
    arrived, arrived_rows = pl.pallas_call(
        functools.partial(exchange_kernel, axes, sizes, spans),
        out_shape=(
            pltpu.VMEM((num_off, slots, num_flux, block_rows), jnp.float32),
            pltpu.VMEM(rows.shape, jnp.int32),
        ),
        in_specs=[hbm, hbm, smem, smem, hbm, hbm],
        out_specs=(vmem, vmem),
        scratch_shapes=[
            pltpu.VMEM((land_blocks, num_steps, num_kinds, tiles, block_cols), tile_flux.dtype),
            pltpu.VMEM((land_blocks, tiles, block_cols), tile_frac.dtype),
            pltpu.VMEM(weights.shape[1:], weights.dtype),
            pltpu.VMEM((num_off, slots, num_flux, block_rows), jnp.float32),
            pltpu.SemaphoreType.DMA((land_blocks,)),
            pltpu.SemaphoreType.DMA((land_blocks,)),
            pltpu.SemaphoreType.DMA((num_off, len(spans))),
            pltpu.SemaphoreType.DMA,
            pltpu.SemaphoreType.DMA((num_off, len(spans))),
            pltpu.SemaphoreType.DMA((num_off, len(spans))),
            pltpu.SemaphoreType.DMA((num_off,)),
            pltpu.SemaphoreType.DMA((num_off,)),
        ],
        compiler_params=pltpu.CompilerParams(collective_id=0, has_side_effects=True,
                                             vmem_limit_bytes=57 * 2**20),
        name="exchange",
    )(tile_flux, tile_frac, columns, send_counts, rows, weights[0])

    out = pl.pallas_call(
        settle_kernel,
        out_shape=jax.ShapeDtypeStruct((num_kinds, num_steps, atm_blocks * block_rows),
                                       jnp.float32),
        in_specs=[vmem, vmem],
        out_specs=hbm,
        scratch_shapes=[
            pltpu.SMEM(rows.shape, jnp.int32),
            pltpu.VMEM((atm_blocks, num_flux, block_rows), jnp.float32),
            pltpu.VMEM((num_kinds, num_steps, atm_blocks * block_rows), jnp.float32),
            pltpu.SemaphoreType.DMA,
            pltpu.SemaphoreType.DMA((OUT_CUTS,)),
        ],
        compiler_params=pltpu.CompilerParams(vmem_limit_bytes=16 * 2**20),
        name="settle",
    )(arrived_rows, arrived)
    return out.transpose(1, 0, 2)


AB_DEV = 48


def solution(mesh):
    axes = ("gx", "gy")
    sizes = (mesh.shape["gx"], mesh.shape["gy"])
    return jax.shard_map(
        functools.partial(on_device, axes, sizes, AB_DEV),
        mesh=mesh,
        in_specs=(
            P(None, None, None, ("gx", "gy")),
            P(None, ("gx", "gy")),
            P(("gx", "gy"), None, None, None, None),
            P(("gx", "gy"), None, None),
            P(("gx", "gy"), None, None),
            P(("gx", "gy"), None),
        ),
        out_specs=P(None, None, ("gx", "gy")),
        check_vma=False,
    )
```

```python
import functools

import jax
import jax.numpy as jnp
from jax import lax
from jax.experimental import pallas as pl
from jax.experimental.pallas import tpu as pltpu
from jax.sharding import PartitionSpec as P

CUTS = 8
OUT_CUTS = 4
EARLY = 4
EDGE = 2


def chunk_spans(slots):
    spans, begin, size = [], 0, max(slots // CUTS, 1)
    while begin < slots:
        size = min(size if begin == 0 else begin, slots - begin)
        spans.append((begin, size))
        begin += size
    return spans


def flow_orders(reach):
    far = list(range(reach, 0, -1))
    both = [sign * away for away in far for sign in (1, -1)]
    down = [-away for away in far] + far
    up = far + [-away for away in far]
    return both, down, up


def send_order(reach, spans):
    order = []
    for stage in range(reach):
        for chunk in range(len(spans)):
            order += [(2 * stage, chunk), (2 * stage + 1, chunk)]
    return order + [(2 * reach, chunk) for chunk in range(len(spans))]


def exchange_kernel(axes, sizes, spans, flux_ref, frac_ref, col_ref, count_ref, rows_ref,
                    weights_ref, arrived_ref, arrived_rows_ref,
                    flux_buf, frac_buf, weights_buf, part_buf, flux_sem, frac_sem, weight_sem,
                    own_sem, send_sem, recv_sem, row_send_sem, row_recv_sem):
    num_off, slots = weights_buf.shape[0], weights_buf.shape[1]
    num_steps, num_kinds, tiles, _ = flux_ref.shape
    cols = weights_buf.shape[3]
    reach = num_off // 2
    inner = sizes[1]
    count = sizes[0] * sizes[1]
    me = lax.axis_index(axes[0]) * inner + lax.axis_index(axes[1])
    order = send_order(reach, spans)
    spot = lax.axis_index(axes[1])
    offsets = [
        reach + jnp.where(spot < EDGE, down, jnp.where(spot >= inner - EDGE, up, both))
        for both, down, up in zip(*flow_orders(reach))
    ] + [reach]
    own = num_off - 1

    def place(offset):
        there = lax.rem(me + offset - reach + count, count)
        return (there // inner, lax.rem(there, inner))

    barrier = pltpu.get_barrier_semaphore()
    for offset in range(num_off):
        if offset != reach:
            pl.semaphore_signal(barrier, inc=1, device_id=place(offset),
                                device_id_type=pl.DeviceIdType.MESH)

    land_loads = []
    for block in range(flux_buf.shape[0]):
        lanes = pl.ds(block * cols, cols)
        land_loads.append(pltpu.make_async_copy(
            flux_ref.at[:, :, :, lanes], flux_buf.at[block], flux_sem.at[block]))
        land_loads.append(pltpu.make_async_copy(
            frac_ref.at[:, lanes], frac_buf.at[block], frac_sem.at[block]))
    for load in land_loads:
        load.start()
    loads = {}
    for flow, chunk in order:
        offset = offsets[flow]
        span = pl.ds(*spans[chunk])
        loads[flow, chunk] = pltpu.make_async_copy(
            weights_ref.at[offset, span], weights_buf.at[offset, span],
            weight_sem.at[flow, chunk])
    for key in order[:EARLY]:
        loads[key].start()

    for load in land_loads:
        load.wait()
    for key in order[EARLY:]:
        loads[key].start()
    copies = []
    for flow, chunk in order:
        offset = offsets[flow]
        begin, size = spans[chunk]
        loads[flow, chunk].wait()
        part_ref = arrived_ref if flow == own else part_buf

        def one_slot(slot, carry, offset=offset, part_ref=part_ref):
            live = jnp.where(slot < count_ref[0, offset], 1.0, 0.0).astype(jnp.float32)
            block = col_ref[offset, 0, slot]
            frac = frac_buf[block]
            flux = flux_buf[block].astype(jnp.float32)
            flux = jnp.stack([flux[step] for step in range(num_steps)], axis=1)
            flux = flux.reshape(num_steps * num_kinds, tiles, cols)
            merged = jnp.sum(flux * frac[None], axis=1) / jnp.sum(frac, axis=0, keepdims=True)
            value = lax.dot_general(merged.astype(jnp.bfloat16), weights_buf[offset, slot],
                                    (((1,), (1,)), ((), ())),
                                    preferred_element_type=jnp.float32)
            part_ref[offset, slot] = value * live
            return carry

        lax.fori_loop(begin, begin + size, one_slot, 0)
        if not copies:
            pl.semaphore_wait(barrier, num_off - 1)
        span = pl.ds(begin, size)
        if flow != own:
            copy = pltpu.make_async_remote_copy(
                src_ref=part_buf.at[offset, span], dst_ref=arrived_ref.at[offset, span],
                send_sem=send_sem.at[offset, chunk], recv_sem=recv_sem.at[offset, chunk],
                device_id=place(offset), device_id_type=pl.DeviceIdType.MESH)
            copy.start()
            copies.append(copy)
        if chunk == 0:
            if flow != own:
                copy = pltpu.make_async_remote_copy(
                    src_ref=rows_ref.at[offset], dst_ref=arrived_rows_ref.at[offset],
                    send_sem=row_send_sem.at[offset], recv_sem=row_recv_sem.at[offset],
                    device_id=place(offset), device_id_type=pl.DeviceIdType.MESH)
            else:
                copy = pltpu.make_async_copy(
                    rows_ref.at[reach], arrived_rows_ref.at[reach], own_sem)
            copy.start()
            copies.append(copy)
    for copy in copies:
        copy.wait()


def settle_kernel(rows_ref, arrived_ref, out_ref, rows, total, out_buf, load_sem, out_sem):
    num_off, slots = arrived_ref.shape[0], arrived_ref.shape[1]
    num_kinds, num_steps = out_ref.shape[0], out_ref.shape[1]
    blocks, _, block_rows = total.shape
    load = pltpu.make_async_copy(rows_ref, rows, load_sem)
    load.start()
    total[...] = jnp.zeros_like(total)
    load.wait()
    for offset in range(num_off):
        def one_slot(slot, carry, offset=offset):
            row = rows[offset, 0, slot]
            total[row] = total[row] + arrived_ref[offset, slot]
            return carry

        lax.fori_loop(0, slots, one_slot, 0, unroll=4)

    per_cut = blocks // OUT_CUTS
    stores = []
    for cut in range(OUT_CUTS):
        def one_block(block, carry):
            lanes = pl.ds(pl.multiple_of(block * block_rows, block_rows), block_rows)
            out_buf[:, :, lanes] = total[block].reshape(num_kinds, num_steps, block_rows)
            return carry

        lax.fori_loop(cut * per_cut, (cut + 1) * per_cut, one_block, 0, unroll=2)
        lanes = pl.ds(cut * per_cut * block_rows, per_cut * block_rows)
        store = pltpu.make_async_copy(
            out_buf.at[:, :, lanes], out_ref.at[:, :, lanes], out_sem.at[cut])
        store.start()
        stores.append(store)
    for store in stores:
        store.wait()


def on_device(axes, sizes, atm_blocks, tile_flux, tile_frac, weights, block_row, block_col,
              send_counts):
    num_steps, num_kinds = tile_flux.shape[0], tile_flux.shape[1]
    num_flux = num_steps * num_kinds
    num_off, slots, block_rows, block_cols = weights.shape[1:]
    tiles = tile_flux.shape[2]
    land_blocks = tile_flux.shape[3] // block_cols
    spans = chunk_spans(slots)
    rows = block_row.transpose(1, 0, 2)
    columns = block_col.transpose(1, 0, 2)

    vmem = pl.BlockSpec(memory_space=pltpu.VMEM)
    smem = pl.BlockSpec(memory_space=pltpu.SMEM)
    hbm = pl.BlockSpec(memory_space=pltpu.HBM)
    arrived, arrived_rows = pl.pallas_call(
        functools.partial(exchange_kernel, axes, sizes, spans),
        out_shape=(
            pltpu.VMEM((num_off, slots, num_flux, block_rows), jnp.float32),
            pltpu.VMEM(rows.shape, jnp.int32),
        ),
        in_specs=[hbm, hbm, smem, smem, hbm, hbm],
        out_specs=(vmem, vmem),
        scratch_shapes=[
            pltpu.VMEM((land_blocks, num_steps, num_kinds, tiles, block_cols), tile_flux.dtype),
            pltpu.VMEM((land_blocks, tiles, block_cols), tile_frac.dtype),
            pltpu.VMEM(weights.shape[1:], weights.dtype),
            pltpu.VMEM((num_off, slots, num_flux, block_rows), jnp.float32),
            pltpu.SemaphoreType.DMA((land_blocks,)),
            pltpu.SemaphoreType.DMA((land_blocks,)),
            pltpu.SemaphoreType.DMA((num_off, len(spans))),
            pltpu.SemaphoreType.DMA,
            pltpu.SemaphoreType.DMA((num_off, len(spans))),
            pltpu.SemaphoreType.DMA((num_off, len(spans))),
            pltpu.SemaphoreType.DMA((num_off,)),
            pltpu.SemaphoreType.DMA((num_off,)),
        ],
        compiler_params=pltpu.CompilerParams(collective_id=0, has_side_effects=True,
                                             vmem_limit_bytes=57 * 2**20),
        name="exchange",
    )(tile_flux, tile_frac, columns, send_counts, rows, weights[0])

    out = pl.pallas_call(
        settle_kernel,
        out_shape=jax.ShapeDtypeStruct((num_kinds, num_steps, atm_blocks * block_rows),
                                       jnp.float32),
        in_specs=[vmem, vmem],
        out_specs=hbm,
        scratch_shapes=[
            pltpu.SMEM(rows.shape, jnp.int32),
            pltpu.VMEM((atm_blocks, num_flux, block_rows), jnp.float32),
            pltpu.VMEM((num_kinds, num_steps, atm_blocks * block_rows), jnp.float32),
            pltpu.SemaphoreType.DMA,
            pltpu.SemaphoreType.DMA((OUT_CUTS,)),
        ],
        compiler_params=pltpu.CompilerParams(vmem_limit_bytes=16 * 2**20),
        name="settle",
    )(arrived_rows, arrived)
    return out.transpose(1, 0, 2)


AB_DEV = 48


def solution(mesh):
    axes = ("gx", "gy")
    sizes = (mesh.shape["gx"], mesh.shape["gy"])
    return jax.shard_map(
        functools.partial(on_device, axes, sizes, AB_DEV),
        mesh=mesh,
        in_specs=(
            P(None, None, None, ("gx", "gy")),
            P(None, ("gx", "gy")),
            P(("gx", "gy"), None, None, None, None),
            P(("gx", "gy"), None, None),
            P(("gx", "gy"), None, None),
            P(("gx", "gy"), None),
        ),
        out_specs=P(None, None, ("gx", "gy")),
        check_vma=False,
    )
```
